32 devices in a mesh: gx: 2 (over x), gy: 4 (over z), gz: 4 (over y, core).
Axes of the slice: x: 2, y: 2, z: 4, core: 2. Of those that a mesh axis runs over, the one named last changes fastest.
Arguments:
- offsets: float32 [3, 4, 16, 4, 256], P(None, 'gx', 'gy', 'gz'), may hold values from 0 to 1
- velocity: float32 [3, 4, 16, 4, 256], P(None, 'gx', 'gy', 'gz'), may hold values from -6 to 6
- mass: float32 [4, 16, 4, 256], P('gx', 'gy', 'gz'), may hold values from 0.004 to 0.04
- counts: int32 [4, 16, 4], P('gx', 'gy', 'gz'), may hold values from 64 to 256
Outputs:
- new_offsets: float32 [3, 4, 16, 4, 256], P(None, 'gx', 'gy', 'gz')
- new_velocity: float32 [3, 4, 16, 4, 256], P(None, 'gx', 'gy', 'gz')
The draws below stay inside these ranges and needn't reach their ends.
Inputs may be any that keep to these rules, and one draw needn't show every extreme that they name: `counts`: slots at or past a leaf's count are padding; their masses and positions carry no meaning as sources.
All inputs are finite; a program needn't handle non-finite values.
Results may differ from the reference program's by a relative error of at most 0.0001.
Values sent between devices are 32-bit elements; how exact they have to be, the bound alone decides.
A program may use at most 64 MiB of HBM per device.

```python
import math
import jax
import jax.numpy as jnp
import numpy as np
from jax import lax

SLOTS = 256
SUBSTEPS = 2
LEAVES_X = 4
LEAVES_Y = 16
LEAVES_Z = 4


def set_ends(result, own_key, smallest, largest):
    longest = result.shape.index(max(result.shape))
    spots = []
    for shift in (0, 1):
        where = [jax.random.randint(jax.random.fold_in(own_key, axis), (), 0, length) for axis, length in enumerate(result.shape)]
        where[longest] = (where[longest] + shift) % result.shape[longest]
        spots.append(tuple(where))
    return result.at[spots[0]].set(smallest).at[spots[1]].set(largest)


def level_of(rng, extent, pieces, least, high):
    gain, own = 1.0, jax.random.fold_in(rng, 6)
    for axis_at, parts in pieces:
        heights = jnp.exp(jax.random.uniform(jax.random.fold_in(own, axis_at), (parts,), jnp.float32, least / len(pieces), high / len(pieces)))
        gain = gain * jnp.repeat(heights, extent[axis_at] // parts).reshape([-1 if axis == axis_at else 1 for axis in range(len(extent))])
    return gain


def noise(key, shape, spread, bound, cuts=(), held_as=jnp.bfloat16):
    gain = level_of(key, shape, cuts, -0.22, 0.18) if cuts else 1.0
    values = jax.random.normal(key, shape, jnp.float32) * spread * gain
    return jnp.minimum(jnp.maximum(values, -bound), bound).astype(held_as)


def setup_inputs(seed: int = 0) -> dict:
    streams_of = jax.random.split(jax.random.key(seed), 5)
    offsets = jnp.clip(1.0 * jax.random.uniform(streams_of[0], (3, LEAVES_X, LEAVES_Y, LEAVES_Z, SLOTS), jnp.float32) ** level_of(streams_of[0], (3, LEAVES_X, LEAVES_Y, LEAVES_Z, SLOTS), ((1, 2), (2, 4), (3, 4)), -0.2, 0.2), 0.0, 1.0)
    velocity = noise(streams_of[1], (3, LEAVES_X, LEAVES_Y, LEAVES_Z, SLOTS), 1.0, 6.0, ((1, 2), (2, 4), (3, 4)), jnp.float32)
    mass = jnp.clip(jnp.exp(math.log(0.04) - 2.30258502 * jax.random.uniform(streams_of[2], (LEAVES_X, LEAVES_Y, LEAVES_Z, SLOTS), jnp.float32) ** level_of(streams_of[2], (LEAVES_X, LEAVES_Y, LEAVES_Z, SLOTS), ((0, 2), (1, 4), (2, 4)), -0.2, 0.2)), 0.004, 0.04)
    counts = set_ends(jax.random.randint(streams_of[3], (LEAVES_X, LEAVES_Y, LEAVES_Z), SLOTS // 4, SLOTS + 1), jax.random.fold_in(streams_of[3], 1), SLOTS // 4, SLOTS).astype(jnp.int32)
    return dict(offsets=offsets, velocity=velocity, mass=mass, counts=counts)


def pair_tile(target, source, shift):
    dist = source[:3, ..., None, :] + shift.reshape((3,) + (1,) * (source.ndim)) - target[..., :, None]
    square = jnp.sum(dist * dist, axis=0)
    factor = (square + 0.01) ** (-1.5) * jnp.maximum(1.0 - square, 0.0) ** 2
    scaled = source[3][..., None, :] * factor
    return jnp.sum(scaled[None] * dist, axis=-1)


def accel(position, weight):
    source = jnp.concatenate([position, weight[None]], axis=0)
    table = jnp.array(np.array([[a, b, c] for a in (-1, 0, 1) for b in (-1, 0, 1) for c in (-1, 0, 1)], dtype=np.int32))

    def one_offset(total, offset):
        rolled = jnp.roll(source, (-offset[0], -offset[1], -offset[2]), axis=(1, 2, 3))
        shift = offset.astype(jnp.float32)
        tiles = lax.map(lambda pair: pair_tile(pair[0], pair[1], shift),
                        (jnp.moveaxis(position, 1, 0), jnp.moveaxis(rolled, 1, 0)))
        return total + jnp.moveaxis(tiles, 0, 1), None

    total, _ = lax.scan(one_offset, jnp.zeros_like(position), table)
    return total


def reference(offsets, velocity, mass, counts):
    slot = jnp.arange(mass.shape[-1], dtype=jnp.int32)
    weight = jnp.where(slot < counts[..., None], mass, jnp.float32(0.0))
    position, speed = offsets, velocity
    for step in range(SUBSTEPS):
        speed = speed + 0.1 * accel(position, weight)
        position = position + 0.1 * speed
    return position, speed
```

```python
import functools

import jax
import jax.numpy as jnp
from jax import lax
from jax.experimental import pallas as pl
from jax.experimental.pallas import tpu as pltpu
from jax.sharding import PartitionSpec as P

SUBSTEPS = 2
WIDE = 256


def with_halo(block, sides, width):
    for axis, dim in sides:
        count = lax.axis_size(axis)
        forward = [(i, i + 1) for i in range(count - 1)]
        forward.append((count - 1, 0))
        backward = [(target, source) for source, target in forward]
        low = lax.ppermute(
            lax.slice_in_dim(block, block.shape[dim] - width, None, axis=dim), axis, forward
        )
        high = lax.ppermute(lax.slice_in_dim(block, 0, width, axis=dim), axis, backward)
        block = jnp.concatenate([low, block, high], axis=dim)
    return block


def split3(tile):
    high = tile.astype(jnp.bfloat16).astype(jnp.float32)
    rest = tile - high
    mid = rest.astype(jnp.bfloat16).astype(jnp.float32)
    return high, mid, rest - mid


def force_kernel(span, counts, src, vel, pos_out, vel_out, pack, tfeat, dist_a, dist_b, acc):
    span_x, span_y, span_z = span
    slots = src.shape[-1]
    row8 = lax.broadcasted_iota(jnp.int32, (8, WIDE), 0)
    lane128 = lax.broadcasted_iota(jnp.int32, (4, 128), 1)
    row4 = lax.broadcasted_iota(jnp.int32, (4, slots), 0)
    pad = 128 - 48
    pack[...] = jnp.zeros_like(pack)

    def one_leaf(leaf, carry):
        at_x = leaf // (span_y * span_z)
        at_y = (leaf // span_z) % span_y
        at_z = leaf % span_z

        def put(tile, off):
            start = pl.multiple_of((off // 128) * 128, 128)
            shift = off % 128
            wide = jnp.concatenate([tile, jnp.zeros((4, 128), jnp.float32)], axis=1)
            wide = pltpu.roll(wide, shift, 1)
            old = pack[0:4, pl.ds(start, 128)]
            pack[0:4, pl.ds(start, 128)] = jnp.where(lane128 < shift, old, wide[:, :128])
            pack[0:4, pl.ds(start + 128, slots)] = wide[:, 128:]

        def one_source(k, off):
            step_x = k // 9
            step_y = (k // 3) % 3
            step_z = k % 3
            tile = src[at_x + step_x, at_y + step_y, at_z + step_z]
            move = jnp.where(
                row4 == 0,
                (step_x - 1).astype(jnp.float32) - 0.5,
                jnp.where(
                    row4 == 1,
                    (step_y - 1).astype(jnp.float32) - 0.5,
                    jnp.where(row4 == 2, (step_z - 1).astype(jnp.float32) - 0.5, 0.0),
                ),
            )
            put(tile + move, off)
            place = ((at_x + step_x) * (span_y + 2) + at_y + step_y) * (span_z + 2) + at_z + step_z
            return off + counts[place]

        total = lax.fori_loop(0, 27, one_source, jnp.int32(0))
        put(jnp.zeros((4, slots), jnp.float32), total)
        pack[0:4, pl.ds(pl.multiple_of((total // 128) * 128, 128) + 384, 2 * WIDE)] = jnp.zeros(
            (4, 2 * WIDE), jnp.float32
        )

        own = src[at_x + 1, at_y + 1, at_z + 1]
        own = jnp.concatenate([own, jnp.zeros((4, slots), jnp.float32)], axis=0)
        rows = lax.broadcasted_iota(jnp.int32, (8, slots), 0)
        centred = jnp.where(rows < 3, own - 0.5, 0.0)
        norm = jnp.sum(centred * centred, axis=0, keepdims=True) + 0.01
        high, mid, low = split3(jnp.where(rows == 4, norm, -2.0 * centred))
        high = high + jnp.where(rows == 3, 1.0, 0.0)
        feats = jnp.concatenate(
            [high, mid, high, mid, low, high, jnp.zeros((pad, slots), jnp.float32)], axis=0
        )
        tfeat[...] = feats.T.astype(jnp.bfloat16)
        acc[...] = jnp.zeros_like(acc)

        def distances(chunk):
            tile = pack[:, pl.ds(pl.multiple_of(chunk * WIDE, WIDE), WIDE)]
            where = jnp.where(row8 < 3, tile, 0.0)
            square = jnp.sum(where * where, axis=0, keepdims=True)
            high, mid, low = split3(
                jnp.where(row8 == 3, square, jnp.where(row8 == 4, 1.0, where))
            )
            feats = jnp.concatenate(
                [high, high, mid, mid, high, low, jnp.zeros((pad, WIDE), jnp.float32)], axis=0
            ).astype(jnp.bfloat16)
            return jnp.dot(tfeat[...], feats, preferred_element_type=jnp.float32)

        def gather(chunk, dist):
            tile = pack[:, pl.ds(pl.multiple_of(chunk * WIDE, WIDE), WIDE)]
            mass = tile[3:4, :]
            terms = [
                jnp.broadcast_to(tile[0:1, :] * mass, (8, WIDE)),
                jnp.broadcast_to(tile[1:2, :] * mass, (8, WIDE)),
                jnp.broadcast_to(tile[2:3, :] * mass, (8, WIDE)),
                jnp.broadcast_to(mass, (8, WIDE)),
            ]
            for group in range(slots // 8):
                spot = slice(8 * group, 8 * group + 8)
                square = dist[spot, :]
                inverse = lax.rsqrt(square)
                edge = jnp.maximum(1.01 - square, 0.0) * inverse
                weight = edge * edge * inverse
                for comp in range(4):
                    part = weight * terms[comp]
                    acc[comp, spot, :] += part[:, :128] + part[:, 128:]

        dist_a[...] = distances(0)

        def two_chunks(pair, carry):
            dist_b[...] = distances(2 * pair + 1)
            gather(2 * pair, dist_a)
            dist_a[...] = distances(2 * pair + 2)
            gather(2 * pair + 1, dist_b)
            return carry

        lax.fori_loop(0, (total + 2 * WIDE - 1) // (2 * WIDE), two_chunks, 0)

        sums = [jnp.sum(acc[comp].T, axis=0, keepdims=True) for comp in range(4)]
        for comp in range(3):
            here = centred[comp : comp + 1]
            pull = sums[comp] - here * sums[3]
            speed = vel[leaf, comp : comp + 1, :] + 0.1 * pull
            vel_out[leaf, comp : comp + 1, :] = speed
            pos_out[leaf, comp : comp + 1, :] = own[comp : comp + 1] + 0.1 * speed
        return carry

    lax.fori_loop(0, span_x * span_y * span_z, one_leaf, 0)


def substep(span, counts, src, vel):
    leaves = span[0] * span[1] * span[2]
    slots = src.shape[-1]
    room = 27 * slots + 4 * WIDE + 512
    vmem = pl.BlockSpec(memory_space=pltpu.VMEM)
    return pl.pallas_call(
        functools.partial(force_kernel, span),
        out_shape=(
            jax.ShapeDtypeStruct((leaves, 3, slots), jnp.float32),
            jax.ShapeDtypeStruct((leaves, 3, slots), jnp.float32),
        ),
        in_specs=[pl.BlockSpec(memory_space=pltpu.SMEM), vmem, vmem],
        out_specs=(vmem, vmem),
        scratch_shapes=[
            pltpu.VMEM((8, room), jnp.float32),
            pltpu.VMEM((slots, 128), jnp.bfloat16),
            pltpu.VMEM((slots, WIDE), jnp.float32),
            pltpu.VMEM((slots, WIDE), jnp.float32),
            pltpu.VMEM((4, slots, 128), jnp.float32),
        ],
        name="forces",
    )(counts, src, vel)


def shards(offsets, velocity, mass, counts):
    slots = mass.shape[-1]
    span = mass.shape[:3]
    sides = (("gz", 2), ("gy", 1), ("gx", 0))
    slot = jnp.arange(slots, dtype=jnp.int32)
    weight = jnp.where(slot < counts[..., None], mass, jnp.float32(0.0))
    position = jnp.moveaxis(offsets, 0, 3)
    speed = jnp.moveaxis(velocity, 0, 3).reshape(-1, 3, slots)
    padded = with_halo(jnp.concatenate([position, weight[..., None, :]], axis=3), sides, 1)
    padded_mass = padded[..., 3:, :]
    live = jnp.max(jnp.where(padded_mass[..., 0, :] > 0, slot + 1, 0), axis=-1).reshape(-1)
    for step in range(SUBSTEPS):
        if step > 0:
            padded = jnp.concatenate([with_halo(position, sides, 1), padded_mass], axis=3)
        position, speed = substep(span, live, padded, speed)
        position = position.reshape(span + (3, slots))
    back = lambda array: jnp.moveaxis(array.reshape(span + (3, slots)), 3, 0)
    return (back(position), back(speed))


def solution(mesh):
    return jax.shard_map(
        shards,
        mesh=mesh,
        in_specs=(
            P(None, "gx", "gy", "gz", None),
            P(None, "gx", "gy", "gz", None),
            P("gx", "gy", "gz", None),
            P("gx", "gy", "gz"),
        ),
        out_specs=(P(None, "gx", "gy", "gz", None), P(None, "gx", "gy", "gz", None)),
        check_vma=False,
    )
```

```python
import functools

import jax
import jax.numpy as jnp
from jax import lax
from jax.experimental import pallas as pl
from jax.experimental.pallas import tpu as pltpu
from jax.sharding import PartitionSpec as P

SUBSTEPS = 2
WIDE = 256


def with_halo(block, sides, width):
    for axis, dim in sides:
        count = lax.axis_size(axis)
        forward = [(i, i + 1) for i in range(count - 1)]
        forward.append((count - 1, 0))
        backward = [(target, source) for source, target in forward]
        low = lax.ppermute(
            lax.slice_in_dim(block, block.shape[dim] - width, None, axis=dim), axis, forward
        )
        high = lax.ppermute(lax.slice_in_dim(block, 0, width, axis=dim), axis, backward)
        block = jnp.concatenate([low, block, high], axis=dim)
    return block


def split3(tile):
    high = tile.astype(jnp.bfloat16).astype(jnp.float32)
    rest = tile - high
    mid = rest.astype(jnp.bfloat16).astype(jnp.float32)
    return high, mid, rest - mid


def force_kernel(span, counts, src, vel, pos_out, vel_out, pack, tfeat, dist_a, dist_b, acc):
    span_x, span_y, span_z = span
    slots = src.shape[-1]
    row8 = lax.broadcasted_iota(jnp.int32, (8, WIDE), 0)
    lane128 = lax.broadcasted_iota(jnp.int32, (4, 128), 1)
    row4 = lax.broadcasted_iota(jnp.int32, (4, slots), 0)
    pad = 128 - 48
    pack[...] = jnp.zeros_like(pack)

    def one_leaf(leaf, carry):
        at_x = leaf // (span_y * span_z)
        at_y = (leaf // span_z) % span_y
        at_z = leaf % span_z

        def put(tile, off):
            shift = lax.bitwise_and(off, 127)
            start = pl.multiple_of(off - shift, 128)
            wide = jnp.concatenate([tile, jnp.zeros((4, 128), jnp.float32)], axis=1)
            wide = pltpu.roll(wide, shift, 1)
            old = pack[0:4, pl.ds(start, 128)]
            pack[0:4, pl.ds(start, 128)] = jnp.where(lane128 < shift, old, wide[:, :128])
            pack[0:4, pl.ds(start + 128, slots)] = wide[:, 128:]

        total = jnp.int32(0)
        for step_x in range(3):
            for step_y in range(3):
                for step_z in range(3):
                    move = jnp.where(
                        row4 == 0,
                        step_x - 1.5,
                        jnp.where(
                            row4 == 1, step_y - 1.5, jnp.where(row4 == 2, step_z - 1.5, 0.0)
                        ),
                    )
                    put(src[at_x + step_x, at_y + step_y, at_z + step_z] + move, total)
                    place = (at_x + step_x) * (span_y + 2) + at_y + step_y
                    total = total + counts[place * (span_z + 2) + at_z + step_z]
        put(jnp.zeros((4, slots), jnp.float32), total)
        pack[0:4, pl.ds(pl.multiple_of(total - lax.bitwise_and(total, 127), 128) + 384, 2 * WIDE)] = jnp.zeros(
            (4, 2 * WIDE), jnp.float32
        )

        own = src[at_x + 1, at_y + 1, at_z + 1]
        own = jnp.concatenate([own, jnp.zeros((4, slots), jnp.float32)], axis=0)
        rows = lax.broadcasted_iota(jnp.int32, (8, slots), 0)
        centred = jnp.where(rows < 3, own - 0.5, 0.0)
        norm = jnp.sum(centred * centred, axis=0, keepdims=True) + 0.01
        high, mid, low = split3(jnp.where(rows == 4, norm, -2.0 * centred))
        high = high + jnp.where(rows == 3, 1.0, 0.0)
        feats = jnp.concatenate(
            [high, mid, high, mid, low, high, jnp.zeros((pad, slots), jnp.float32)], axis=0
        )
        tfeat[...] = feats.T.astype(jnp.bfloat16)
        acc[...] = jnp.zeros_like(acc)

        def distances(chunk):
            tile = pack[:, pl.ds(pl.multiple_of(chunk * WIDE, WIDE), WIDE)]
            where = jnp.where(row8 < 3, tile, 0.0)
            square = jnp.sum(where * where, axis=0, keepdims=True)
            high, mid, low = split3(
                jnp.where(row8 == 3, square, jnp.where(row8 == 4, 1.0, where))
            )
            feats = jnp.concatenate(
                [high, high, mid, mid, high, low, jnp.zeros((pad, WIDE), jnp.float32)], axis=0
            ).astype(jnp.bfloat16)
            return jnp.dot(tfeat[...], feats, preferred_element_type=jnp.float32)

        def gather(chunk, dist):
            tile = pack[:, pl.ds(pl.multiple_of(chunk * WIDE, WIDE), WIDE)]
            mass = tile[3:4, :]
            terms = [
                jnp.broadcast_to(tile[0:1, :] * mass, (8, WIDE)),
                jnp.broadcast_to(tile[1:2, :] * mass, (8, WIDE)),
                jnp.broadcast_to(tile[2:3, :] * mass, (8, WIDE)),
                jnp.broadcast_to(mass, (8, WIDE)),
            ]
            for group in range(slots // 8):
                spot = slice(8 * group, 8 * group + 8)
                square = dist[spot, :]
                inverse = lax.rsqrt(square)
                edge = jnp.maximum(1.01 - square, 0.0) * inverse
                weight = edge * edge * inverse
                for comp in range(4):
                    part = weight * terms[comp]
                    acc[comp, spot, :] += part[:, :128] + part[:, 128:]

        dist_a[...] = distances(0)

        def two_chunks(pair, carry):
            dist_b[...] = distances(2 * pair + 1)
            gather(2 * pair, dist_a)
            dist_a[...] = distances(2 * pair + 2)
            gather(2 * pair + 1, dist_b)
            return carry

        lax.fori_loop(0, (total + 2 * WIDE - 1) // (2 * WIDE), two_chunks, 0)

        sums = [jnp.sum(acc[comp].T, axis=0, keepdims=True) for comp in range(4)]
        for comp in range(3):
            here = centred[comp : comp + 1]
            pull = sums[comp] - here * sums[3]
            speed = vel[leaf, comp : comp + 1, :] + 0.1 * pull
            vel_out[leaf, comp : comp + 1, :] = speed
            pos_out[leaf, comp : comp + 1, :] = own[comp : comp + 1] + 0.1 * speed
        return carry

    lax.fori_loop(0, span_x * span_y * span_z, one_leaf, 0)


def substep(span, counts, src, vel):
    leaves = span[0] * span[1] * span[2]
    slots = src.shape[-1]
    room = 27 * slots + 4 * WIDE + 512
    vmem = pl.BlockSpec(memory_space=pltpu.VMEM)
    return pl.pallas_call(
        functools.partial(force_kernel, span),
        out_shape=(
            jax.ShapeDtypeStruct((leaves, 3, slots), jnp.float32),
            jax.ShapeDtypeStruct((leaves, 3, slots), jnp.float32),
        ),
        in_specs=[pl.BlockSpec(memory_space=pltpu.SMEM), vmem, vmem],
        out_specs=(vmem, vmem),
        scratch_shapes=[
            pltpu.VMEM((8, room), jnp.float32),
            pltpu.VMEM((slots, 128), jnp.bfloat16),
            pltpu.VMEM((slots, WIDE), jnp.float32),
            pltpu.VMEM((slots, WIDE), jnp.float32),
            pltpu.VMEM((4, slots, 128), jnp.float32),
        ],
        name="forces",
    )(counts, src, vel)


def shards(offsets, velocity, mass, counts):
    slots = mass.shape[-1]
    span = mass.shape[:3]
    sides = (("gz", 2), ("gy", 1), ("gx", 0))
    slot = jnp.arange(slots, dtype=jnp.int32)
    weight = jnp.where(slot < counts[..., None], mass, jnp.float32(0.0))
    position = jnp.moveaxis(offsets, 0, 3)
    speed = jnp.moveaxis(velocity, 0, 3).reshape(-1, 3, slots)
    padded = with_halo(jnp.concatenate([position, weight[..., None, :]], axis=3), sides, 1)
    padded_mass = padded[..., 3:, :]
    live = jnp.max(jnp.where(padded_mass[..., 0, :] > 0, slot + 1, 0), axis=-1).reshape(-1)
    for step in range(SUBSTEPS):
        if step > 0:
            padded = jnp.concatenate([with_halo(position, sides, 1), padded_mass], axis=3)
        position, speed = substep(span, live, padded, speed)
        position = position.reshape(span + (3, slots))
    back = lambda array: jnp.moveaxis(array.reshape(span + (3, slots)), 3, 0)
    return (back(position), back(speed))


def solution(mesh):
    return jax.shard_map(
        shards,
        mesh=mesh,
        in_specs=(
            P(None, "gx", "gy", "gz", None),
            P(None, "gx", "gy", "gz", None),
            P("gx", "gy", "gz", None),
            P("gx", "gy", "gz"),
        ),
        out_specs=(P(None, "gx", "gy", "gz", None), P(None, "gx", "gy", "gz", None)),
        check_vma=False,
    )
```

```python
import functools
import itertools

import jax
import jax.numpy as jnp
from jax import lax
from jax.experimental import pallas as pl
from jax.experimental.pallas import tpu as pltpu
from jax.sharding import PartitionSpec as P

SUBSTEPS = 2
WIDE = 256
GRANT = 8 << 20


def halo_kernel(axes, sizes, block, padded, send_sems, recv_sems):
    span = block.shape[:3]
    here = [lax.axis_index(axis) for axis in axes]

    def device(step):
        return tuple(
            lax.rem(here[k] + step[k] + sizes[k], sizes[k]) for k in range(3)
        )

    greeted = [
        step
        for step in itertools.product(*[(0, 1) if size == 2 else (-1, 0, 1) for size in sizes])
        if any(step)
    ]
    barrier = pltpu.get_barrier_semaphore()
    for step in greeted:
        pl.semaphore_signal(
            barrier, inc=1, device_id=device(step), device_id_type=pl.DeviceIdType.MESH
        )
    pl.semaphore_wait(barrier, len(greeted))

    steps = [step for step in itertools.product((-1, 0, 1), repeat=3) if any(step)]
    steps.sort(key=lambda step: -sum(abs(part) for part in step))
    copies = []
    for at, step in enumerate(steps):
        source = []
        target = []
        for k in range(3):
            if step[k] == 0:
                source.append(pl.ds(0, span[k]))
                target.append(pl.ds(1, span[k]))
            elif step[k] == 1:
                source.append(pl.ds(span[k] - 1, 1))
                target.append(pl.ds(0, 1))
            else:
                source.append(pl.ds(0, 1))
                target.append(pl.ds(span[k] + 1, 1))
        copy = pltpu.make_async_remote_copy(
            src_ref=block.at[tuple(source)],
            dst_ref=padded.at[tuple(target)],
            send_sem=send_sems.at[at],
            recv_sem=recv_sems.at[at],
            device_id=device(step),
            device_id_type=pl.DeviceIdType.MESH,
        )
        copy.start()
        copies.append(copy)
    padded[1 : span[0] + 1, 1 : span[1] + 1, 1 : span[2] + 1] = block[...]
    for copy in copies:
        copy.wait()


def with_halo(mesh_axes, sizes, block, ident):
    shape = tuple(size + 2 for size in block.shape[:3]) + block.shape[3:]
    vmem = pl.BlockSpec(memory_space=pltpu.VMEM)
    return pl.pallas_call(
        functools.partial(halo_kernel, mesh_axes, sizes),
        out_shape=jax.ShapeDtypeStruct(shape, block.dtype),
        in_specs=[vmem],
        out_specs=vmem,
        scratch_shapes=[pltpu.SemaphoreType.DMA((26,)), pltpu.SemaphoreType.DMA((26,))],
        compiler_params=pltpu.CompilerParams(
            collective_id=ident, has_side_effects=True, vmem_limit_bytes=GRANT
        ),
        name="halo",
    )(block)


def split3(tile):
    high = tile.astype(jnp.bfloat16).astype(jnp.float32)
    rest = tile - high
    mid = rest.astype(jnp.bfloat16).astype(jnp.float32)
    return high, mid, rest - mid


def force_kernel(span, last, counts, src, vel, pos_out, vel_out, pack, tfeat, dist_a, dist_b, acc):
    span_x, span_y, span_z = span
    slots = src.shape[-1]
    row8 = lax.broadcasted_iota(jnp.int32, (8, WIDE), 0)
    lane128 = lax.broadcasted_iota(jnp.int32, (4, 128), 1)
    row4 = lax.broadcasted_iota(jnp.int32, (4, slots), 0)
    pad = 128 - 48
    pack[...] = jnp.zeros_like(pack)

    def one_leaf(leaf, carry):
        at_x = leaf // (span_y * span_z)
        at_y = (leaf // span_z) % span_y
        at_z = leaf % span_z

        def put(tile, off):
            shift = lax.bitwise_and(off, 127)
            start = pl.multiple_of(off - shift, 128)
            wide = jnp.concatenate([tile, jnp.zeros((4, 128), jnp.float32)], axis=1)
            wide = pltpu.roll(wide, shift, 1)
            old = pack[0:4, pl.ds(start, 128)]
            pack[0:4, pl.ds(start, 128)] = jnp.where(lane128 < shift, old, wide[:, :128])
            pack[0:4, pl.ds(start + 128, slots)] = wide[:, 128:]

        total = jnp.int32(0)
        for step_x in range(3):
            for step_y in range(3):
                for step_z in range(3):
                    move = jnp.where(
                        row4 == 0,
                        step_x - 1.5,
                        jnp.where(
                            row4 == 1, step_y - 1.5, jnp.where(row4 == 2, step_z - 1.5, 0.0)
                        ),
                    )
                    put(src[at_x + step_x, at_y + step_y, at_z + step_z] + move, total)
                    place = (at_x + step_x) * (span_y + 2) + at_y + step_y
                    total = total + counts[place * (span_z + 2) + at_z + step_z]
        put(jnp.zeros((4, slots), jnp.float32), total)
        pack[0:4, pl.ds(pl.multiple_of(total - lax.bitwise_and(total, 127), 128) + 384, 2 * WIDE)] = jnp.zeros(
            (4, 2 * WIDE), jnp.float32
        )

        own = src[at_x + 1, at_y + 1, at_z + 1]
        own = jnp.concatenate([own, jnp.zeros((4, slots), jnp.float32)], axis=0)
        rows = lax.broadcasted_iota(jnp.int32, (8, slots), 0)
        centred = jnp.where(rows < 3, own - 0.5, 0.0)
        norm = jnp.sum(centred * centred, axis=0, keepdims=True) + 0.01
        high, mid, low = split3(jnp.where(rows == 4, norm, -2.0 * centred))
        high = high + jnp.where(rows == 3, 1.0, 0.0)
        feats = jnp.concatenate(
            [high, mid, high, mid, low, high, jnp.zeros((pad, slots), jnp.float32)], axis=0
        )
        tfeat[...] = feats.T.astype(jnp.bfloat16)
        acc[...] = jnp.zeros_like(acc)

        def distances(chunk):
            tile = pack[:, pl.ds(pl.multiple_of(chunk * WIDE, WIDE), WIDE)]
            where = jnp.where(row8 < 3, tile, 0.0)
            square = jnp.sum(where * where, axis=0, keepdims=True)
            high, mid, low = split3(
                jnp.where(row8 == 3, square, jnp.where(row8 == 4, 1.0, where))
            )
            feats = jnp.concatenate(
                [high, high, mid, mid, high, low, jnp.zeros((pad, WIDE), jnp.float32)], axis=0
            ).astype(jnp.bfloat16)
            return jnp.dot(tfeat[...], feats, preferred_element_type=jnp.float32)

        def gather(chunk, dist):
            tile = pack[:, pl.ds(pl.multiple_of(chunk * WIDE, WIDE), WIDE)]
            mass = tile[3:4, :]
            terms = [
                jnp.broadcast_to(tile[0:1, :] * mass, (8, WIDE)),
                jnp.broadcast_to(tile[1:2, :] * mass, (8, WIDE)),
                jnp.broadcast_to(tile[2:3, :] * mass, (8, WIDE)),
                jnp.broadcast_to(mass, (8, WIDE)),
            ]
            for group in range(slots // 8):
                spot = slice(8 * group, 8 * group + 8)
                square = dist[spot, :]
                inverse = lax.rsqrt(square)
                edge = jnp.maximum(1.01 - square, 0.0) * inverse
                weight = edge * edge * inverse
                for comp in range(4):
                    part = weight * terms[comp]
                    acc[comp, spot, :] += part[:, :128] + part[:, 128:]

        dist_a[...] = distances(0)

        def two_chunks(pair, carry):
            dist_b[...] = distances(2 * pair + 1)
            gather(2 * pair, dist_a)
            dist_a[...] = distances(2 * pair + 2)
            gather(2 * pair + 1, dist_b)
            return carry

        lax.fori_loop(0, (total + 2 * WIDE - 1) // (2 * WIDE), two_chunks, 0)

        sums = [jnp.sum(acc[comp].T, axis=0, keepdims=True) for comp in range(4)]
        for comp in range(3):
            here = centred[comp : comp + 1]
            pull = sums[comp] - here * sums[3]
            speed = vel[comp, at_x, at_y, pl.ds(at_z, 1), :] + 0.1 * pull
            vel_out[comp, at_x, at_y, pl.ds(at_z, 1), :] = speed
            moved = own[comp : comp + 1] + 0.1 * speed
            if last:
                pos_out[comp, at_x, at_y, pl.ds(at_z, 1), :] = moved
            else:
                pos_out[at_x, at_y, at_z, comp : comp + 1, :] = moved
        if not last:
            pos_out[at_x, at_y, at_z, 3:4, :] = own[3:4]
        return carry

    lax.fori_loop(0, span_x * span_y * span_z, one_leaf, 0)


def substep(span, last, counts, src, vel):
    slots = src.shape[-1]
    room = 27 * slots + 4 * WIDE + 512
    vmem = pl.BlockSpec(memory_space=pltpu.VMEM)
    native = jax.ShapeDtypeStruct(vel.shape, jnp.float32)
    return pl.pallas_call(
        functools.partial(force_kernel, span, last),
        out_shape=(
            native if last else jax.ShapeDtypeStruct(span + (4, slots), jnp.float32),
            native,
        ),
        in_specs=[pl.BlockSpec(memory_space=pltpu.SMEM), vmem, vmem],
        out_specs=(vmem, vmem),
        compiler_params=pltpu.CompilerParams(vmem_limit_bytes=GRANT),
        scratch_shapes=[
            pltpu.VMEM((8, room), jnp.float32),
            pltpu.VMEM((slots, 128), jnp.bfloat16),
            pltpu.VMEM((slots, WIDE), jnp.float32),
            pltpu.VMEM((slots, WIDE), jnp.float32),
            pltpu.VMEM((4, slots, 128), jnp.float32),
        ],
        name="forces",
    )(counts, src, vel)


def shards(axes, sizes, offsets, velocity, mass, counts):
    slots = mass.shape[-1]
    span = mass.shape[:3]
    slot = jnp.arange(slots, dtype=jnp.int32)
    weight = jnp.where(slot < counts[..., None], mass, jnp.float32(0.0))
    position = jnp.concatenate([jnp.moveaxis(offsets, 0, 3), weight[..., None, :]], axis=3)
    speed = velocity
    for step in range(SUBSTEPS):
        padded = with_halo(axes, sizes, position, step)
        if step == 0:
            live = jnp.max(jnp.where(padded[..., 3, :] > 0, slot + 1, 0), axis=-1).reshape(-1)
        position, speed = substep(span, step == SUBSTEPS - 1, live, padded, speed)
    return (position, speed)


def solution(mesh):
    axes = tuple(mesh.axis_names)
    sizes = tuple(mesh.shape[axis] for axis in axes)
    return jax.shard_map(
        functools.partial(shards, axes, sizes),
        mesh=mesh,
        in_specs=(
            P(None, "gx", "gy", "gz", None),
            P(None, "gx", "gy", "gz", None),
            P("gx", "gy", "gz", None),
            P("gx", "gy", "gz"),
        ),
        out_specs=(P(None, "gx", "gy", "gz", None), P(None, "gx", "gy", "gz", None)),
        check_vma=False,
    )
```

```python
import functools
import itertools

import jax
import jax.numpy as jnp
from jax import lax
from jax.experimental import pallas as pl
from jax.experimental.pallas import tpu as pltpu
from jax.sharding import PartitionSpec as P

SUBSTEPS = 2
WIDE = 256
GRANT = 8 << 20


def halo_kernel(axes, sizes, block, padded, send_sems, recv_sems):
    span = block.shape[:3]
    here = [lax.axis_index(axis) for axis in axes]

    def device(step):
        return tuple(
            lax.rem(here[k] + step[k] + sizes[k], sizes[k]) for k in range(3)
        )

    greeted = [
        step
        for step in itertools.product(*[(0, 1) if size == 2 else (-1, 0, 1) for size in sizes])
        if any(step)
    ]
    barrier = pltpu.get_barrier_semaphore()
    for step in greeted:
        pl.semaphore_signal(
            barrier, inc=1, device_id=device(step), device_id_type=pl.DeviceIdType.MESH
        )
    pl.semaphore_wait(barrier, len(greeted))

    steps = [step for step in itertools.product((-1, 0, 1), repeat=3) if any(step)]
    steps.sort(key=lambda step: -sum(abs(part) for part in step))
    copies = []
    for at, step in enumerate(steps):
        source = []
        target = []
        for k in range(3):
            if step[k] == 0:
                source.append(pl.ds(0, span[k]))
                target.append(pl.ds(1, span[k]))
            elif step[k] == 1:
                source.append(pl.ds(span[k] - 1, 1))
                target.append(pl.ds(0, 1))
            else:
                source.append(pl.ds(0, 1))
                target.append(pl.ds(span[k] + 1, 1))
        copy = pltpu.make_async_remote_copy(
            src_ref=block.at[tuple(source)],
            dst_ref=padded.at[tuple(target)],
            send_sem=send_sems.at[at],
            recv_sem=recv_sems.at[at],
            device_id=device(step),
            device_id_type=pl.DeviceIdType.MESH,
        )
        copy.start()
        copies.append(copy)
    padded[1 : span[0] + 1, 1 : span[1] + 1, 1 : span[2] + 1] = block[...]
    for copy in copies:
        copy.wait()


def with_halo(mesh_axes, sizes, block, ident):
    shape = tuple(size + 2 for size in block.shape[:3]) + block.shape[3:]
    vmem = pl.BlockSpec(memory_space=pltpu.VMEM)
    return pl.pallas_call(
        functools.partial(halo_kernel, mesh_axes, sizes),
        out_shape=jax.ShapeDtypeStruct(shape, block.dtype),
        in_specs=[vmem],
        out_specs=vmem,
        scratch_shapes=[pltpu.SemaphoreType.DMA((26,)), pltpu.SemaphoreType.DMA((26,))],
        compiler_params=pltpu.CompilerParams(
            collective_id=ident, has_side_effects=True, vmem_limit_bytes=GRANT
        ),
        name="halo",
    )(block)


def split3(tile):
    high = tile.astype(jnp.bfloat16).astype(jnp.float32)
    rest = tile - high
    mid = rest.astype(jnp.bfloat16).astype(jnp.float32)
    return high, mid, rest - mid


def force_kernel(span, last, counts, src, vel, pos_out, vel_out, pack, tfeat, dist_a, dist_b, held_a, held_b, acc):
    span_x, span_y, span_z = span
    slots = src.shape[-1]
    row8 = lax.broadcasted_iota(jnp.int32, (8, WIDE), 0)
    lane128 = lax.broadcasted_iota(jnp.int32, (4, 128), 1)
    row4 = lax.broadcasted_iota(jnp.int32, (4, slots), 0)
    pad = 128 - 48
    pack[...] = jnp.zeros_like(pack)

    def one_leaf(leaf, carry):
        at_x = leaf // (span_y * span_z)
        at_y = (leaf // span_z) % span_y
        at_z = leaf % span_z

        def put(tile, off):
            shift = lax.bitwise_and(off, 127)
            start = pl.multiple_of(off - shift, 128)
            wide = jnp.concatenate([tile, jnp.zeros((4, 128), jnp.float32)], axis=1)
            wide = pltpu.roll(wide, shift, 1)
            old = pack[0:4, pl.ds(start, 128)]
            pack[0:4, pl.ds(start, 128)] = jnp.where(lane128 < shift, old, wide[:, :128])
            pack[0:4, pl.ds(start + 128, slots)] = wide[:, 128:]

        total = jnp.int32(0)
        for step_x in range(3):
            for step_y in range(3):
                for step_z in range(3):
                    move = jnp.where(
                        row4 == 0,
                        step_x - 1.5,
                        jnp.where(
                            row4 == 1, step_y - 1.5, jnp.where(row4 == 2, step_z - 1.5, 0.0)
                        ),
                    )
                    put(src[at_x + step_x, at_y + step_y, at_z + step_z] + move, total)
                    place = (at_x + step_x) * (span_y + 2) + at_y + step_y
                    total = total + counts[place * (span_z + 2) + at_z + step_z]
        put(jnp.zeros((4, slots), jnp.float32), total)
        pack[0:4, pl.ds(pl.multiple_of(total - lax.bitwise_and(total, 127), 128) + 384, 4 * WIDE)] = jnp.zeros(
            (4, 4 * WIDE), jnp.float32
        )

        own = src[at_x + 1, at_y + 1, at_z + 1]
        own = jnp.concatenate([own, jnp.zeros((4, slots), jnp.float32)], axis=0)
        rows = lax.broadcasted_iota(jnp.int32, (8, slots), 0)
        centred = jnp.where(rows < 3, own - 0.5, 0.0)
        norm = jnp.sum(centred * centred, axis=0, keepdims=True) + 0.01
        high, mid, low = split3(jnp.where(rows == 4, norm, -2.0 * centred))
        high = high + jnp.where(rows == 3, 1.0, 0.0)
        feats = jnp.concatenate(
            [high, mid, high, mid, low, high, jnp.zeros((pad, slots), jnp.float32)], axis=0
        )
        tfeat[...] = feats.T.astype(jnp.bfloat16)
        acc[...] = jnp.zeros_like(acc)

        def distances(chunk):
            tile = pack[:, pl.ds(pl.multiple_of(chunk * WIDE, WIDE), WIDE)]
            where = jnp.where(row8 < 3, tile, 0.0)
            square = jnp.sum(where * where, axis=0, keepdims=True)
            high, mid, low = split3(
                jnp.where(row8 == 3, square, jnp.where(row8 == 4, 1.0, where))
            )
            feats = jnp.concatenate(
                [high, high, mid, mid, high, low, jnp.zeros((pad, WIDE), jnp.float32)], axis=0
            ).astype(jnp.bfloat16)
            return jnp.dot(tfeat[...], feats, preferred_element_type=jnp.float32)

        def weights(dist, out):
            for group in range(slots // 16):
                spot = slice(16 * group, 16 * group + 16)
                square = dist[spot, :]
                inverse = lax.rsqrt(square)
                edge = jnp.maximum(1.01 - square, 0.0) * inverse
                weight = edge * edge * inverse
                high = weight.astype(jnp.bfloat16)
                out[spot, :WIDE] = high
                out[spot, WIDE:] = (weight - high.astype(jnp.float32)).astype(jnp.bfloat16)

        def gather(chunk, held):
            tile = pack[:, pl.ds(pl.multiple_of(chunk * WIDE, WIDE), WIDE)]
            mass = tile[3:4, :]
            parts = jnp.where(row8 < 3, tile * mass, jnp.where(row8 == 3, tile, 0.0))
            high, mid, low = split3(parts)
            stack = jnp.concatenate([high, mid, low, jnp.zeros_like(low)], axis=0)
            stack = stack.astype(jnp.bfloat16)
            acc[...] += lax.dot_general(
                held[...],
                jnp.concatenate([stack, stack], axis=1),
                (((1,), (1,)), ((), ())),
                preferred_element_type=jnp.float32,
            )

        dist_a[...] = distances(0)
        held_b[...] = jnp.zeros_like(held_b)

        def chunks(first, pairs):
            gather(jnp.maximum(first - 1, 0), held_b)
            for pair in range(pairs):
                chunk = first + 2 * pair
                dist_b[...] = distances(chunk + 1)
                weights(dist_a, held_a)
                gather(chunk, held_a)
                dist_a[...] = distances(chunk + 2)
                weights(dist_b, held_b)
                if pair < pairs - 1:
                    gather(chunk + 1, held_b)

        def four_chunks(quad, carry):
            chunks(4 * quad, 2)
            return carry

        def two_chunks(pair, carry):
            chunks(2 * pair, 1)
            return carry

        quads = total // (4 * WIDE)
        pairs = (total + 2 * WIDE - 1) // (2 * WIDE)
        lax.fori_loop(0, quads, four_chunks, 0)
        lax.fori_loop(2 * quads, pairs, two_chunks, 0)
        gather(jnp.maximum(2 * pairs - 1, 0), held_b)

        flat = acc[...].T
        flat = flat[0:8] + flat[8:16] + flat[16:24]
        sums = [flat[comp : comp + 1] for comp in range(4)]
        for comp in range(3):
            here = centred[comp : comp + 1]
            pull = sums[comp] - here * sums[3]
            speed = vel[comp, at_x, at_y, pl.ds(at_z, 1), :] + 0.1 * pull
            vel_out[comp, at_x, at_y, pl.ds(at_z, 1), :] = speed
            moved = own[comp : comp + 1] + 0.1 * speed
            if last:
                pos_out[comp, at_x, at_y, pl.ds(at_z, 1), :] = moved
            else:
                pos_out[at_x, at_y, at_z, comp : comp + 1, :] = moved
        if not last:
            pos_out[at_x, at_y, at_z, 3:4, :] = own[3:4]
        return carry

    lax.fori_loop(0, span_x * span_y * span_z, one_leaf, 0)


def substep(span, last, counts, src, vel):
    slots = src.shape[-1]
    room = 27 * slots + 6 * WIDE + 512
    vmem = pl.BlockSpec(memory_space=pltpu.VMEM)
    native = jax.ShapeDtypeStruct(vel.shape, jnp.float32)
    return pl.pallas_call(
        functools.partial(force_kernel, span, last),
        out_shape=(
            native if last else jax.ShapeDtypeStruct(span + (4, slots), jnp.float32),
            native,
        ),
        in_specs=[pl.BlockSpec(memory_space=pltpu.SMEM), vmem, vmem],
        out_specs=(vmem, vmem),
        compiler_params=pltpu.CompilerParams(vmem_limit_bytes=GRANT),
        scratch_shapes=[
            pltpu.VMEM((8, room), jnp.float32),
            pltpu.VMEM((slots, 128), jnp.bfloat16),
            pltpu.VMEM((slots, WIDE), jnp.float32),
            pltpu.VMEM((slots, WIDE), jnp.float32),
            pltpu.VMEM((slots, 2 * WIDE), jnp.bfloat16),
            pltpu.VMEM((slots, 2 * WIDE), jnp.bfloat16),
            pltpu.VMEM((slots, 32), jnp.float32),
        ],
        name="forces",
    )(counts, src, vel)


def shards(axes, sizes, offsets, velocity, mass, counts):
    slots = mass.shape[-1]
    span = mass.shape[:3]
    slot = jnp.arange(slots, dtype=jnp.int32)
    weight = jnp.where(slot < counts[..., None], mass, jnp.float32(0.0))
    position = jnp.concatenate([jnp.moveaxis(offsets, 0, 3), weight[..., None, :]], axis=3)
    speed = velocity
    for step in range(SUBSTEPS):
        padded = with_halo(axes, sizes, position, step)
        if step == 0:
            live = jnp.max(jnp.where(padded[..., 3, :] > 0, slot + 1, 0), axis=-1).reshape(-1)
        position, speed = substep(span, step == SUBSTEPS - 1, live, padded, speed)
    return (position, speed)


def solution(mesh):
    axes = tuple(mesh.axis_names)
    sizes = tuple(mesh.shape[axis] for axis in axes)
    return jax.shard_map(
        functools.partial(shards, axes, sizes),
        mesh=mesh,
        in_specs=(
            P(None, "gx", "gy", "gz", None),
            P(None, "gx", "gy", "gz", None),
            P("gx", "gy", "gz", None),
            P("gx", "gy", "gz"),
        ),
        out_specs=(P(None, "gx", "gy", "gz", None), P(None, "gx", "gy", "gz", None)),
        check_vma=False,
    )
```
